32 devices in a mesh: grp: 4 (over z), tile: 8 (over y, x, core).
Axes of the slice: x: 2, y: 2, z: 4, core: 2. Of those that a mesh axis runs over, the one named last changes fastest.
Arguments:
- noise: bfloat16 [16, 3, 2048, 2048], P('grp', None, 'tile'), may hold values from -6 to 6
- stress: float32 [6, 2048, 2048], P(None, 'tile', 'grp'), as said below
- timescale: float32 [2048, 2048], P('tile', 'grp'), may hold values from 3 to 256
- mean_inflow: float32 [2048, 2048], P('tile', 'grp'), may hold values from 0.5 to 1.5
- courant: float32 [2048, 2048], P('tile', 'grp'), may hold values from 0.2 to 0.9
- prior_state: float32 [3, 2048, 2048], P(None, 'tile', 'grp'), may hold values from -6 to 6
- field: float32 [3, 8, 2048, 2048], P(None, None, 'tile', 'grp'), may hold values from -6 to 6
Outputs:
- inflow: bfloat16 [16, 3, 2048, 2048], P(None, None, 'tile', 'grp')
- field_out: float32 [3, 8, 2048, 2048], P(None, None, 'tile', 'grp')
The draws below stay inside these ranges and needn't reach their ends.
Inputs may be any that keep to these rules, and one draw needn't show every extreme that they name: stress holds, per cell, R11, R21, R22, R31, R32, R33 of a symmetric positive definite tensor whose Cholesky factor has diagonal entries of 0.3 or more.
All inputs are finite; a program needn't handle non-finite values.
Results may differ from the reference program's by a relative error of at most 0.0085.
Values may be sent and summed in bfloat16 or wider, within the bound.
A program may use at most 128 MiB of HBM per device.

```python
import math
import jax
import jax.numpy as jnp
from jax import lax

NY = 2048
NZ = 2048
LS = 2
FW = 4
CX = 8
PLANES = 16


def draw_stress(key, part):
    diag_key = jax.random.fold_in(key, 11)
    lower_key = jax.random.fold_in(key, 23)
    smallest, largest, reach = (0.3, 1.5, 0.6)
    diagonal = jnp.exp(jax.random.uniform(diag_key, (3, NZ, NY), jnp.float32, math.log(smallest), math.log(largest)))
    lower = jax.random.uniform(lower_key, (3, NZ, NY), jnp.float32, -reach, reach)
    first_diag, second_diag, third_diag = (diagonal[0], diagonal[1], diagonal[2])
    second_low, third_low, third_mid = (lower[0], lower[1], lower[2])
    return jnp.stack([first_diag * first_diag, second_low * first_diag, second_low * second_low + second_diag * second_diag, third_low * first_diag, third_low * second_low + third_mid * second_diag, third_low * third_low + third_mid * third_mid + third_diag * third_diag]).astype(jnp.float32)


def block_scale(key, dims, cuts, low, high):
    loudness, own = 1.0, jax.random.fold_in(key, 6)
    for dim, shards_of in cuts:
        heights = jnp.exp(jax.random.uniform(jax.random.fold_in(own, dim), (shards_of,), jnp.float32, low / len(cuts), high / len(cuts)))
        loudness = loudness * jnp.repeat(heights, dims[dim] // shards_of).reshape([-1 if axis == dim else 1 for axis in range(len(dims))])
    return loudness


def normal_values(own_key, extent, spread, bound, split=(), held_as=jnp.bfloat16):
    result = spread * jax.random.normal(own_key, extent, jnp.float32)
    if split:
        result = result * block_scale(own_key, extent, split, -0.22, 0.18)
    return jnp.clip(result, -bound, bound).astype(held_as)


def setup_inputs(seed: int = 0) -> dict:
    key_of = jax.random.split(jax.random.key(seed), 8)
    noise = normal_values(key_of[0], (PLANES, 3, NY, NZ), 1.0, 6.0, ((0, 4), (2, 8)))
    stress = draw_stress(jax.random.fold_in(key_of[7], 71), 0)
    timescale = jnp.clip(jnp.exp(math.log(256.0) - 4.446565 * jax.random.uniform(key_of[2], (NZ, NY), jnp.float32) ** block_scale(key_of[2], (NZ, NY), ((0, 8), (1, 4)), -0.2, 0.2)), 3.0, 256.0)
    mean_inflow = jnp.clip(0.5 + 1.0 * jax.random.uniform(key_of[3], (NZ, NY), jnp.float32) ** block_scale(key_of[3], (NZ, NY), ((0, 8), (1, 4)), -0.2, 0.2), 0.5, 1.5)
    courant = jnp.clip(jnp.exp(math.log(0.9) - 1.50407736 * jax.random.uniform(key_of[4], (NZ, NY), jnp.float32) ** block_scale(key_of[4], (NZ, NY), ((0, 8), (1, 4)), -0.2, 0.2)), 0.2, 0.9)
    prior_state = normal_values(key_of[5], (3, NZ, NY), 1.0, 6.0, ((1, 8), (2, 4)), jnp.float32)
    field = normal_values(key_of[6], (3, CX, NZ, NY), 1.0, 6.0, ((2, 8), (3, 4)), jnp.float32)
    return dict(noise=noise, stress=stress, timescale=timescale, mean_inflow=mean_inflow, courant=courant, prior_state=prior_state, field=field)


def filter_taps():
    offsets = jnp.arange(-FW, FW + 1).astype(jnp.float32)
    raw = jnp.exp(-math.pi * offsets * offsets / (2.0 * LS * LS))
    return (raw / jnp.sqrt(jnp.sum(raw * raw))).astype(jnp.bfloat16)

def cholesky_cells(stress):
    first_diag = jnp.sqrt(stress[0])
    second_low = stress[1] / first_diag
    second_diag = jnp.sqrt(stress[2] - second_low * second_low)
    third_low = stress[3] / first_diag
    third_mid = (stress[4] - second_low * third_low) / second_diag
    third_diag = jnp.sqrt(stress[5] - third_low * third_low - third_mid * third_mid)
    return (first_diag, second_low, second_diag, third_low, third_mid, third_diag)

def velocity_of(state, factors, mean_inflow):
    first_diag, second_low, second_diag, third_low, third_mid, third_diag = factors
    return jnp.stack([mean_inflow + first_diag * state[0], second_low * state[0] + second_diag * state[1], third_low * state[0] + third_mid * state[1] + third_diag * state[2]])

def march(current, courant, velocity):
    upstream = jnp.concatenate([velocity[:, None], current[:, :-1]], axis=1)
    return (1.0 - courant) * current + courant * upstream

def reference(noise, stress, timescale, mean_inflow, courant, prior_state, field):
    taps = filter_taps().astype(jnp.float32)
    decay = jnp.exp(-math.pi / (2.0 * timescale))
    gain = jnp.sqrt(1.0 - decay * decay)
    factors = cholesky_cells(stress)

    def one_plane(carry, plane):
        state, current = carry
        span = jnp.zeros(plane.shape, jnp.float32)
        for offset in range(2 * FW + 1):
            span = span + taps[offset] * jnp.roll(plane, FW - offset, axis=2).astype(jnp.float32)
        rounded = lax.optimization_barrier(span.astype(jnp.bfloat16))
        padded = jnp.pad(rounded, ((0, 0), (FW, FW), (0, 0))).astype(jnp.float32)
        filtered = jnp.zeros(plane.shape, jnp.float32)
        for offset in range(2 * FW + 1):
            filtered = filtered + taps[offset] * padded[:, offset:offset + NY, :]
        state = decay * state + gain * jnp.swapaxes(filtered, 1, 2)
        velocity = velocity_of(state, factors, mean_inflow)
        current = march(current, courant, velocity)
        return ((state, current), velocity.astype(jnp.bfloat16))
    (state, current), inflow = lax.scan(one_plane, (prior_state, field), noise)
    return (inflow, current)
```

```python
import functools
import math

import jax
import jax.numpy as jnp
import numpy as np
from jax import lax
from jax.experimental import pallas as pl
from jax.experimental.pallas import tpu as pltpu
from jax.sharding import PartitionSpec as P


LS = 2
FW = 4
LANES = 128
SUB = 16
LAG = 4
SHARES = (2, 2, 4, 4, 3, 1)
MESH = pl.DeviceIdType.MESH
CONTRACT_LAST = (((1,), (1,)), ((), ()))


def chunk_sizes(rows):
    units, rest = divmod(rows, SUB)
    if rest:
        return (rows,)
    if units % sum(SHARES) == 0:
        return tuple(share * SUB * (units // sum(SHARES)) for share in SHARES)
    parts = math.gcd(units, 4)
    return (rows // parts,) * parts


def filter_taps():
    offsets = np.arange(-FW, FW + 1).astype(np.float32)
    raw = np.exp(-math.pi * offsets * offsets / np.float32(2.0 * LS * LS)).astype(np.float32)
    return (raw / np.sqrt(np.sum(raw * raw))).astype(jnp.bfloat16)


def band_weights(height, width, first):
    distance = np.arange(width)[None, :] - first - np.arange(height)[:, None]
    taps = filter_taps()
    held = taps[np.clip(distance + FW, 0, 2 * FW)]
    return np.where(np.abs(distance) <= FW, held, np.zeros((), jnp.bfloat16))


def span_windows(rows, devices, offset, chunk):
    starts, leads = [], []
    for t in range(devices):
        at = t * rows + offset
        low = (at - FW) // LANES * LANES
        starts.append(low)
        leads.append(at - low)
    width = -(-(max(leads) + chunk + FW) // LANES) * LANES
    kinds = sorted(set(leads))
    weights = np.stack([band_weights(chunk, width, lead) for lead in kinds])
    return [(low, kinds.index(lead)) for low, lead in zip(starts, leads)], weights


def front_kernel(
    windows, groups, band, noise_ref, zw_ref, yw_ref, *rest
):
    out_refs = rest[:groups]
    sent, got, order, send_sem, recv_sem = rest[groups:]
    total, devices, chunk, _ = got.shape
    width = zw_ref.shape[2]
    block = yw_ref.shape[0]
    step = pl.program_id(0)
    me = lax.axis_index("tile")
    group = lax.axis_index("grp")
    barrier = pltpu.get_barrier_semaphore()

    @pl.when(step == 0)
    def _():
        for hop in range(1, devices):
            peer = lax.rem(me + hop, devices)
            pl.semaphore_signal(barrier, inc=1, device_id={"tile": peer}, device_id_type=MESH)

    @pl.when(step == 1)
    def _():
        pl.semaphore_wait(barrier, devices - 1)

    @pl.when(jnp.logical_and(step >= 1, step <= total))
    def _():
        item = step - 1
        for hop in range(1, devices):
            peer = lax.rem(me + hop, devices)
            pltpu.make_async_remote_copy(
                src_ref=sent.at[item, peer],
                dst_ref=got.at[item, me],
                send_sem=send_sem.at[item],
                recv_sem=recv_sem.at[item],
                device_id={"tile": peer},
                device_id_type=MESH,
            ).start()

    @pl.when(step < total)
    def _():
        length = noise_ref.shape[3]
        for t, (low, kind) in enumerate(windows):
            pieces = []
            at = low
            while at < low + width:
                begin = at % length
                run = min(low + width - at, length - begin)
                pieces.append(noise_ref[0, 0, :, begin : begin + run])
                at += run
            window = pieces[0] if len(pieces) == 1 else jnp.concatenate(pieces, axis=1)
            value = lax.dot_general(
                zw_ref[kind], window, CONTRACT_LAST, preferred_element_type=jnp.float32
            )
            sent[step, t] = value.astype(jnp.bfloat16)

    @pl.when(step >= LAG)
    def _():
        item = step - LAG
        arrived = got.at[item, pl.ds(0, devices - 1)]
        pltpu.make_async_copy(arrived, arrived, recv_sem.at[item]).wait()
        got[item, me] = sent[item, me]
        x = jnp.concatenate([got[item, t] for t in range(devices)], axis=1)
        length = x.shape[1]
        zeros = jnp.zeros((chunk, LANES), x.dtype)
        tall = []
        for start in range(0, length, block):
            after = start + block
            tall.append(
                jnp.concatenate(
                    [
                        x[:, start - LANES : start] if start else zeros,
                        x[:, start:after],
                        x[:, after : after + LANES] if after < length else zeros,
                    ],
                    axis=1,
                )
            )
        value = lax.dot_general(
            jnp.concatenate(tall, axis=0),
            yw_ref[...],
            CONTRACT_LAST,
            preferred_element_type=jnp.float32,
        ).astype(jnp.bfloat16)
        for i, start in enumerate(range(0, length, block)):
            owner, inner = divmod(start, band)
            ahead = lax.rem(owner - group + groups, groups)
            order[ahead, :, inner : inner + block] = value[i * chunk : (i + 1) * chunk]
        for ahead in range(groups):
            out_refs[ahead][0, 0] = order[ahead]

    @pl.when(step == total + LAG - 1)
    def _():
        for item in range(total):
            gone = sent.at[item, pl.ds(0, devices - 1)]
            pltpu.make_async_copy(gone, gone, send_sem.at[item]).wait()


def march_kernel(planes, cells, groups, group_ref, *refs):
    parts, refs = refs[:groups], refs[groups:]
    stress_ref, time_ref, mean_ref, cour_ref, prior_ref, field_ref = refs[:6]
    inflow_ref, result_ref, vel_ref, filt_ref = refs[-4:]
    lanes = mean_ref.shape[1]
    steps = planes // groups
    for behind in range(groups):
        source = lax.rem(group_ref[0] - behind + groups, groups)
        for p in range(steps):
            filt_ref[source * steps + p] = parts[behind][p]

    @pl.loop(0, lanes // LANES)
    def _(tile):
        at = pl.ds(pl.multiple_of(tile * LANES, LANES), LANES)
        decay = jnp.exp(-math.pi / (2.0 * time_ref[:, at]))
        gain = jnp.sqrt(1.0 - decay * decay)
        d1 = jnp.sqrt(stress_ref[0, :, at])
        l21 = stress_ref[1, :, at] / d1
        d2 = jnp.sqrt(stress_ref[2, :, at] - l21 * l21)
        l31 = stress_ref[3, :, at] / d1
        l32 = (stress_ref[4, :, at] - l21 * l31) / d2
        d3 = jnp.sqrt(stress_ref[5, :, at] - l31 * l31 - l32 * l32)
        mean = mean_ref[:, at]
        s0, s1, s2 = (prior_ref[c, :, at] for c in range(3))
        for p in range(planes):
            f0, f1, f2 = (filt_ref[p, c, :, at].astype(jnp.float32) for c in range(3))
            s0 = decay * s0 + gain * f0
            s1 = decay * s1 + gain * f1
            s2 = decay * s2 + gain * f2
            velocity = (mean + d1 * s0, l21 * s0 + d2 * s1, l31 * s0 + l32 * s1 + d3 * s2)
            for c in range(3):
                vel_ref[p, c] = velocity[c]
                inflow_ref[p, c, :, at] = velocity[c].astype(jnp.bfloat16)
        courant = cour_ref[:, at]
        keep = 1.0 - courant
        for c in range(3):
            current = [field_ref[c, x, :, at] for x in range(cells)]
            for p in range(planes):
                moved = [courant * value for value in current[:-1]]
                moved.insert(0, courant * vel_ref[p, c])
                current = [keep * value + up for value, up in zip(current, moved)]
            for x in range(cells):
                result_ref[c, x, :, at] = current[x]


def body(noise, stress, timescale, mean_inflow, courant, prior_state, field):
    devices, groups = lax.axis_size("tile"), lax.axis_size("grp")
    steps, comps, yrows, length = noise.shape
    rows, band = mean_inflow.shape
    planes = steps * groups
    cells = field.shape[1]
    sizes = chunk_sizes(rows)
    unit = SUB if rows % SUB == 0 else rows
    block = math.gcd(band, 256)
    total = steps * comps
    yw = band_weights(block, block + 2 * LANES, LANES)
    group = lax.axis_index("grp").astype(jnp.int32).reshape(1)
    scalar = pl.BlockSpec(memory_space=pltpu.SMEM)

    def front_of(k, offset, chunk):
        windows, zw = span_windows(rows, devices, offset, chunk)

        def source(i):
            item = jnp.minimum(i, total - 1)
            return (item // comps, item % comps, 0, 0)

        def target(i):
            item = jnp.maximum(i - LAG, 0)
            return (item // comps, item % comps, 0, 0)

        moved = total * (devices - 1) * chunk * yrows * 2
        return pl.pallas_call(
            functools.partial(front_kernel, windows, groups, band),
            grid=(total + LAG,),
            in_specs=[
                pl.BlockSpec((1, 1, yrows, length), source),
                pl.BlockSpec(zw.shape, lambda i: (0, 0, 0)),
                pl.BlockSpec(yw.shape, lambda i: (0, 0)),
            ],
            out_specs=[pl.BlockSpec((1, 1, chunk, band), target) for _ in range(groups)],
            out_shape=[
                jax.ShapeDtypeStruct((steps, comps, chunk, band), jnp.bfloat16)
                for _ in range(groups)
            ],
            scratch_shapes=[
                pltpu.VMEM((total, devices, chunk, yrows), jnp.bfloat16),
                pltpu.VMEM((total, devices, chunk, yrows), jnp.bfloat16),
                pltpu.VMEM((groups, chunk, band), jnp.bfloat16),
                pltpu.SemaphoreType.DMA((total,)),
                pltpu.SemaphoreType.DMA((total,)),
            ],
            compiler_params=pltpu.CompilerParams(collective_id=k, has_side_effects=True),
            cost_estimate=pl.CostEstimate(
                flops=4 * total * chunk * length * 512,
                bytes_accessed=2 * noise.size + 4 * moved,
                transcendentals=0,
            ),
            name="front",
        )(noise, zw, yw)

    def march_of(offset, chunk, parts, outs):
        first = offset // unit

        def here(*lead):
            dims = tuple(lead) + (unit, band)
            return pl.BlockSpec(dims, lambda i, n=len(lead): (0,) * n + (first + i, 0))

        specs = [scalar]
        specs += [pl.BlockSpec((steps, comps, unit, band), lambda i: (0, 0, i, 0))] * groups
        specs += [here(6), here(), here(), here(), here(comps), here(comps, cells)]
        args = [group, *parts, stress, timescale, mean_inflow, courant, prior_state, field]
        aliases = {}
        if outs is not None:
            aliases = {len(args): 0, len(args) + 1: 1}
            specs = specs + [pl.BlockSpec(memory_space=pl.ANY)] * 2
            args = args + list(outs)
        return pl.pallas_call(
            functools.partial(march_kernel, planes, cells, groups),
            grid=(chunk // unit,),
            in_specs=specs,
            out_specs=[here(planes, comps), here(comps, cells)],
            out_shape=[
                jax.ShapeDtypeStruct((planes, comps, rows, band), jnp.bfloat16),
                jax.ShapeDtypeStruct(field.shape, jnp.float32),
            ],
            scratch_shapes=[
                pltpu.VMEM((planes, comps, unit, LANES), jnp.float32),
                pltpu.VMEM((planes, comps, unit, band), jnp.bfloat16),
            ],
            input_output_aliases=aliases,
            cost_estimate=pl.CostEstimate(
                flops=100 * planes * chunk * band,
                bytes_accessed=chunk * band * (4 * planes * comps + 8 * comps * cells + 48),
                transcendentals=0,
            ),
            name="march",
        )(*args)

    ready, offset = [], 0
    for k, chunk in enumerate(sizes):
        filtered = front_of(k, offset, chunk)
        ready.append((offset, chunk, exchange(filtered, groups)))
        offset += chunk
    outs = None
    for offset, chunk, parts in ready:
        outs = march_of(offset, chunk, parts, outs)
    return tuple(outs)


def exchange(blocks, groups):
    received = [blocks[0]]
    for d in range(1, groups):
        received.append(
            lax.ppermute(blocks[d], "grp", [(i, (i + d) % groups) for i in range(groups)])
        )
    return received


def solution(mesh):
    placed = (
        P("grp", None, "tile", None),
        P(None, "tile", "grp"),
        P("tile", "grp"),
        P("tile", "grp"),
        P("tile", "grp"),
        P(None, "tile", "grp"),
        P(None, None, "tile", "grp"),
    )

    return jax.shard_map(
        body,
        mesh=mesh,
        in_specs=placed,
        out_specs=(P(None, None, "tile", "grp"), P(None, None, "tile", "grp")),
        check_vma=False,
    )
```
